32 devices in a mesh: dp: 4 (over y, core), vocab: 8 (over z, x).
Axes of the slice: x: 2, y: 2, z: 4, core: 2. Of those that a mesh axis runs over, the one named last changes fastest.
Arguments:
- hidden: bfloat16 [768, 8192], P('dp', 'vocab'), may hold values from -100 to 100
- proj: bfloat16 [8192, 65536], P(None, ('dp', 'vocab')), may hold values from -3 to 3
- target_ids: int32 [768], replicated, may hold values from 0 to 65535
- seq_len: int32 [16], replicated, may hold values from 1 to 189, as said below
- seq_way: int32 [16], replicated, may hold values from 0 to 3
Outputs:
- token_logprob: float32 [768], P('dp')
- token_entropy: float32 [768], P('dp')
- seq_logprob: float32 [16], replicated
The draws below stay inside these ranges and needn't reach their ends.
Inputs may be any that keep to these rules, and one draw needn't show every extreme that they name: `seq_len`: each data way is given exactly 4 sequences, which fill its first slots one after another in increasing sequence number; the lengths on one way add up to at most 192, to exactly 192 on some way, and over all ways to exactly 372. Some sequence has exactly 189 tokens.
All inputs are finite; a program needn't handle non-finite values.
Results may differ from the reference program's by a relative error of at most 0.0003.
Values may be sent and summed in bfloat16 or wider, within the bound.
No kernel may reach another device: no remote copies, remote signals or barrier semaphores. Data moves between devices by JAX's collectives and lax.ppermute only.
A program may use at most 128 MiB of HBM per device.

```python
import math
import jax
import jax.numpy as jnp
from jax import lax

D = 8192
V = 65536
CAP = 192
SEQ_DEV = 4
ROWS = 768
N_DP = 4


def sequence_plan(key):
    base = jax.random.fold_in(key, 101)
    count = SEQ_DEV * N_DP
    others = N_DP - 1
    full = jax.random.randint(jax.random.fold_in(base, 1), (), 0, N_DP)
    ways = jnp.arange(N_DP, dtype=jnp.int32)
    rank = (ways - full - 1) % N_DP
    tilt = jax.random.randint(jax.random.fold_in(base, 2), (N_DP,), 0, 3 * CAP // 32 + 1)
    following = jnp.where(rank + 1 < others, rank + 1, 0)
    extra = 3 * CAP // 16 + tilt[rank] - tilt[following]
    loads = jnp.where(rank < others, CAP // 8 + extra, CAP)
    weights = jax.random.randint(jax.random.fold_in(base, 3), (N_DP, SEQ_DEV), 1, 17)
    spare = loads - SEQ_DEV
    parts = weights * spare[:, None] // jnp.sum(weights, axis=1)[:, None]
    lengths = 1 + parts
    lengths = lengths.at[:, 0].add(loads - jnp.sum(lengths, axis=1))
    full_lengths = jnp.ones((SEQ_DEV,), jnp.int32).at[0].set(CAP - SEQ_DEV + 1)
    lengths = jnp.where((rank < others)[:, None], lengths.astype(jnp.int32), full_lengths[None, :])
    order = jax.random.permutation(jax.random.fold_in(base, 4), count)
    flat_way = jnp.arange(count, dtype=jnp.int32) // SEQ_DEV
    seq_way = jnp.zeros((count,), jnp.int32).at[order].set(flat_way)
    seq_len = jnp.zeros((count,), jnp.int32).at[order].set(lengths.reshape(-1).astype(jnp.int32))
    return (seq_len, seq_way)


def draw_seq_len(key, part):
    return sequence_plan(key)[0]


def draw_seq_way(key, part):
    return sequence_plan(key)[1]


def draw_proj(key, part):
    values = jnp.clip(jax.random.normal(jax.random.fold_in(key, 303), (D, V), jnp.float32), -6.0, 6.0) * (3.0 / math.sqrt(D))
    return values.astype(jnp.bfloat16)


def draw_hidden(key, part):
    values = jnp.clip(jax.random.normal(jax.random.fold_in(key, 404), (CAP * N_DP, D), jnp.float32), -6.0, 6.0)
    return values.astype(jnp.bfloat16)


def plant(drawn, own_key, smallest, high):
    index_at = [jax.random.randint(jax.random.fold_in(own_key, axis), (), 0, length) for axis, length in enumerate(drawn.shape)]
    widest = drawn.shape.index(max(drawn.shape))
    neighbour = index_at[:widest] + [(index_at[widest] + 1) % drawn.shape[widest]] + index_at[widest + 1:]
    return drawn.at[tuple(index_at)].set(smallest).at[tuple(neighbour)].set(high)


def setup_inputs(seed: int = 0) -> dict:
    streams_of = jax.random.split(jax.random.key(seed), 6)
    return {
        "hidden": draw_hidden(jax.random.fold_in(streams_of[5], 71), 0),
        "proj": draw_proj(jax.random.fold_in(streams_of[5], 71), 0),
        "target_ids": plant(jax.random.randint(streams_of[2], (ROWS,), 0, V), jax.random.fold_in(streams_of[2], 1), 0, V - 1).astype(jnp.int32),
        "seq_len": draw_seq_len(jax.random.fold_in(streams_of[5], 71), 0),
        "seq_way": draw_seq_way(jax.random.fold_in(streams_of[5], 71), 0),
    }


floor_value = -1.0e30


def membership(seq_len, seq_way, slots, ways):
    count = seq_len.shape[0]
    order = jnp.arange(count, dtype=jnp.int32)
    earlier = (seq_way[:, None] == seq_way[None, :]) & (order[:, None] < order[None, :])
    start = jnp.sum(jnp.where(earlier, seq_len[:, None], 0), axis=0).astype(jnp.int32)
    row = jnp.arange(slots * ways, dtype=jnp.int32)
    owner = row // slots
    within = row % slots
    return (seq_way[None, :] == owner[:, None]) & (within[:, None] >= start[None, :]) & (within[:, None] < (start + seq_len)[None, :])


def local_stats(logits, first_col, targets):
    top = jnp.max(logits, axis=1)
    shifted = logits - top[:, None]
    weight = jnp.exp(shifted)
    total = jnp.sum(weight, axis=1)
    moment = jnp.sum(weight * shifted, axis=1)
    columns = first_col + jnp.arange(logits.shape[1], dtype=jnp.int32)
    picked = jnp.sum(jnp.where(targets[:, None] == columns[None, :], logits, 0.0), axis=1)
    return top, total, moment, picked


def combine_stats(early, later):
    top = jnp.maximum(early[0], later[0])
    scale_early = jnp.exp(early[0] - top)
    scale_later = jnp.exp(later[0] - top)
    total = early[1] * scale_early + later[1] * scale_later
    moment = scale_early * (early[2] + early[1] * (early[0] - top)) + scale_later * (later[2] + later[1] * (later[0] - top))
    return top, total, moment, early[3] + later[3]


def reference(hidden, proj, target_ids, seq_len, seq_way):
    member = membership(seq_len, seq_way, CAP, N_DP)
    valid = jnp.any(member, axis=1)
    block = math.gcd(V, 4096)
    count = hidden.shape[0]

    def step(carry, index):
        start = (index * block).astype(jnp.int32)
        columns = lax.dynamic_slice_in_dim(proj, start, block, 1)
        logits = jnp.dot(hidden, columns, preferred_element_type=jnp.float32)
        return combine_stats(carry, local_stats(logits, start, target_ids)), None

    zeros = jnp.zeros((count,), jnp.float32)
    init = (jnp.full((count,), floor_value, jnp.float32), zeros, zeros, zeros)
    stats, _ = lax.scan(step, init, jnp.arange(V // block, dtype=jnp.int32))
    top, total, moment, picked = stats
    log_total = jnp.log(total)
    token_logprob = jnp.where(valid, picked - top - log_total, 0.0)
    token_entropy = jnp.where(valid, log_total - moment / total, 0.0)
    seq_logprob = jnp.dot(member.astype(jnp.float32).T, token_logprob, precision=lax.Precision.HIGHEST)
    return token_logprob, token_entropy, seq_logprob
```

```python
import functools

import jax
import jax.numpy as jnp
from jax import lax
from jax.experimental import pallas as pl
from jax.experimental.pallas import tpu as pltpu
from jax.sharding import PartitionSpec as P


AXES = ("dp", "vocab")
CHUNKS = 2
PAIR = 2
FLOOR = -1.0e30


def round_up(value, step):
    return -(-value // step) * step


def estimate(flops, moved):
    return pl.CostEstimate(flops=flops, bytes_accessed=moved, transcendentals=0)


def params(mib):
    return pltpu.CompilerParams(vmem_limit_bytes=mib * 1024 * 1024)


def whole_spec(shape):
    return pl.BlockSpec(shape, lambda *_: (0,) * len(shape))


def compact_kernel(rows, ids, offs, lens, *refs):
    pieces, out = refs[:-1], refs[-1]
    slots = pieces[0].shape[0]
    gap = lax.broadcasted_iota(jnp.int32, (rows, slots), 0) - lax.broadcasted_iota(jnp.int32, (rows, slots), 1)
    slot = lax.broadcasted_iota(jnp.int32, (rows, slots), 1)
    total = None
    for k, piece in enumerate(pieces):
        way = ids[k]
        hot = (gap == offs[way]) & (slot < lens[way])
        part = jnp.dot(
            jnp.where(hot, 1.0, 0.0).astype(jnp.bfloat16), piece[...], preferred_element_type=jnp.float32
        )
        total = part if total is None else total + part
    out[...] = total.astype(jnp.bfloat16)


def compact(rows, ids, offs, lens, pieces):
    slots, depth = pieces[0].shape
    return pl.pallas_call(
        functools.partial(compact_kernel, rows),
        grid_spec=pltpu.PrefetchScalarGridSpec(
            num_scalar_prefetch=3,
            grid=(1,),
            in_specs=[whole_spec(piece.shape) for piece in pieces],
            out_specs=whole_spec((rows, depth)),
        ),
        out_shape=jax.ShapeDtypeStruct((rows, depth), jnp.bfloat16),
        compiler_params=params(16),
        cost_estimate=estimate(2 * rows * slots * depth * len(pieces), 4 * rows * depth),
        name="compact",
    )(ids, offs, lens, *pieces)


def target_kernel(rows, offs, lens, first, ids, out):
    ways, slots = ids.shape
    gap = lax.broadcasted_iota(jnp.int32, (rows, slots), 0) - lax.broadcasted_iota(jnp.int32, (rows, slots), 1)
    slot = lax.broadcasted_iota(jnp.int32, (rows, slots), 1)
    total = jnp.full((rows, slots), 0, jnp.int32)
    for way in range(ways):
        hot = (gap == offs[way]) & (slot < lens[way])
        total += jnp.where(hot, ids[way : way + 1, :] - first[0], 0)
    out[...] = jnp.broadcast_to(jnp.sum(total, axis=1, keepdims=True), out.shape)


def compact_targets(rows, offs, lens, first, ids):
    return pl.pallas_call(
        functools.partial(target_kernel, rows),
        grid_spec=pltpu.PrefetchScalarGridSpec(
            num_scalar_prefetch=3,
            grid=(1,),
            in_specs=[whole_spec(ids.shape)],
            out_specs=whole_spec((rows, 128)),
        ),
        out_shape=jax.ShapeDtypeStruct((rows, 128), jnp.int32),
        compiler_params=params(16),
        cost_estimate=estimate(1000000, 400000),
        name="targets",
    )(offs, lens, first, ids)


def product(lefts, weights):
    total = None
    depth = lefts[0].shape[1]
    for k, left in enumerate(lefts):
        part = jnp.dot(left[...], weights[k * depth : (k + 1) * depth, :], preferred_element_type=jnp.float32)
        total = part if total is None else total + part
    return total


def block_kernel(groups, chunks, started, blocks, *refs):
    lefts = [refs[g * chunks : (g + 1) * chunks] for g in range(groups)]
    weights = refs[groups * chunks : groups * chunks + groups]
    total = product(lefts[0], weights[0])
    for g in range(1, groups):
        total += product(lefts[g], weights[g])
    if started:
        total += refs[-2][...]
    refs[-1][...] = total


def block_product(groups, blocks, proj, tile, carry):
    chunks = len(groups[0])
    rows, depth = groups[0][0].shape
    width = proj.shape[1]
    full = depth * chunks
    in_specs = [whole_spec((rows, depth))] * (len(groups) * chunks)
    for g in range(len(groups)):
        in_specs.append(pl.BlockSpec((full, tile), lambda n, ids, g=g: (ids[g], n)))
    operands = [left for group in groups for left in group] + [proj] * len(groups)
    alias = {}
    if carry is not None:
        in_specs.append(pl.BlockSpec((rows, tile), lambda n, ids: (0, n)))
        alias = {len(operands) + 1: 0}
        operands.append(carry)
    return pl.pallas_call(
        functools.partial(block_kernel, len(groups), chunks, carry is not None),
        grid_spec=pltpu.PrefetchScalarGridSpec(
            num_scalar_prefetch=1,
            grid=(width // tile,),
            in_specs=in_specs,
            out_specs=pl.BlockSpec((rows, tile), lambda n, ids: (0, n)),
        ),
        out_shape=jax.ShapeDtypeStruct((rows, width), jnp.float32),
        input_output_aliases=alias,
        compiler_params=params(20),
        cost_estimate=estimate(2 * rows * full * width * len(groups), 2 * full * width * len(groups)),
        name="block",
    )(blocks, *operands)


def last_kernel(chunks, half, blocks, *refs):
    mine, other = refs[:chunks], refs[chunks : 2 * chunks]
    weights, carry, targets, out, left, top_ref, total_ref, moment_ref, pick_ref = refs[2 * chunks :]
    step = pl.program_id(0)
    tile = weights.shape[1]

    @pl.when(step == 0)
    def _():
        core = blocks[1]
        depth = mine[0].shape[1]
        here = pl.ds(pl.multiple_of(core * half, half), half)
        there = pl.ds(pl.multiple_of((1 - core) * half, half), half)
        for k in range(chunks):
            left[here, k * depth : (k + 1) * depth] = mine[k][...]
            left[there, k * depth : (k + 1) * depth] = other[k][...]
        top_ref[...] = jnp.full(top_ref.shape, FLOOR, jnp.float32)
        total_ref[...] = jnp.zeros(total_ref.shape, jnp.float32)
        moment_ref[...] = jnp.zeros(moment_ref.shape, jnp.float32)
        pick_ref[...] = jnp.zeros(pick_ref.shape, jnp.float32)

    logits = carry[...] + jnp.dot(left[...], weights[...], preferred_element_type=jnp.float32)
    before = top_ref[...]
    top = jnp.maximum(before, jnp.max(logits, axis=1, keepdims=True))
    shifted = logits - top
    weight = jnp.exp(shifted)
    drop = before - top
    scale = jnp.exp(drop)
    column = lax.broadcasted_iota(jnp.int32, logits.shape, 1) + step * tile
    hit = jnp.where(column == targets[:, 0:1], logits, 0.0)
    earlier = total_ref[...]
    moment_ref[...] = scale * (moment_ref[...] + earlier * drop) + jnp.sum(weight * shifted, axis=1, keepdims=True)
    total_ref[...] = scale * earlier + jnp.sum(weight, axis=1, keepdims=True)
    pick_ref[...] = pick_ref[...] + jnp.sum(hit, axis=1, keepdims=True)
    top_ref[...] = top

    @pl.when(step == pl.num_programs(0) - 1)
    def _():
        lane = lax.broadcasted_iota(jnp.int32, (top_ref.shape[0], 128), 1)
        packed = jnp.where(lane == 0, top_ref[...], 0.0)
        packed = jnp.where(lane == 1, total_ref[...], packed)
        packed = jnp.where(lane == 2, moment_ref[...], packed)
        packed = jnp.where(lane == 3, pick_ref[...], packed)
        out[...] = jnp.transpose(packed)[: out.shape[0], :]


def last_product(mine, other, blocks, proj, tile, carry, targets):
    chunks = len(mine)
    half, depth = mine[0].shape
    rows, width = carry.shape
    full = depth * chunks
    in_specs = [whole_spec((half, depth))] * (2 * chunks)
    in_specs.append(pl.BlockSpec((full, tile), lambda n, ids: (ids[0], n)))
    in_specs.append(pl.BlockSpec((rows, tile), lambda n, ids: (0, n)))
    in_specs.append(whole_spec(targets.shape))
    return pl.pallas_call(
        functools.partial(last_kernel, chunks, half),
        grid_spec=pltpu.PrefetchScalarGridSpec(
            num_scalar_prefetch=1,
            grid=(width // tile,),
            in_specs=in_specs,
            out_specs=whole_spec((4, rows)),
            scratch_shapes=[pltpu.VMEM((rows, full), jnp.bfloat16)] + [pltpu.VMEM((rows, 1), jnp.float32)] * 4,
        ),
        out_shape=jax.ShapeDtypeStruct((4, rows), jnp.float32),
        compiler_params=params(20),
        cost_estimate=estimate(2 * rows * full * width, 2 * full * width + 4 * rows * width),
        name="last",
    )(blocks, *mine, *other, proj, carry, targets)


def per_device(hidden, proj, target_ids, seq_len, seq_way):
    ways, size = lax.axis_size("dp"), lax.axis_size("vocab")
    slots, depth = hidden.shape
    width = proj.shape[1]
    spots, ring = ways // PAIR, size // PAIR
    kept = slots + (ways - 1) * (5 * slots // 16)
    rows = round_up(kept, 32)
    half = rows // 2
    piece = depth // CHUNKS
    tile = min(512, width)
    dp, vocab = lax.axis_index("dp"), lax.axis_index("vocab")
    spot, core = dp // PAIR, dp % PAIR
    hop, side = vocab // PAIR, vocab % PAIR

    def swap(value):
        return lax.ppermute(value, "dp", [(i, i ^ 1) for i in range(ways)])

    def turn(value, k):
        return lax.ppermute(value, "dp", [(i, (i + k * PAIR) % ways) for i in range(ways)])

    def advance(value):
        pairs = []
        for d in range(ways):
            for v in range(size):
                to = (v ^ 1) if d % PAIR == 0 else (v + PAIR) % size
                pairs.append((d * size + v, d * size + to))
        return lax.ppermute(value, AXES, pairs)

    chunks = [hidden[:, k * piece : (k + 1) * piece] for k in range(CHUNKS)]
    turned = [[turn(chunk, k) for k in range(1, spots)] for chunk in chunks]
    gathered = []
    for chunk, more in zip(chunks, turned):
        pieces = [chunk, swap(chunk)]
        for value in more:
            pieces += [value, swap(value)]
        gathered.append(pieces)
    way_of = []
    for k in range(spots):
        there = (spot + spots - k) % spots
        way_of += [there * PAIR + core, there * PAIR + (1 - core)]
    way_of = jnp.stack(way_of).astype(jnp.int32)

    order = jnp.arange(seq_len.shape[0], dtype=jnp.int32)
    way = jnp.arange(ways, dtype=jnp.int32)
    lens = jnp.sum(jnp.where(seq_way[None, :] == way[:, None], seq_len[None, :], 0), axis=1)
    offs = jnp.sum(jnp.where(way[None, :] < way[:, None], lens[None, :], 0), axis=1)
    ahead = (seq_way[None, :] < seq_way[:, None]) | (
        (seq_way[None, :] == seq_way[:, None]) & (order[None, :] < order[:, None])
    )
    begin = jnp.sum(jnp.where(ahead, seq_len[None, :], 0), axis=1)
    first = (vocab + dp * size) * width
    targets = compact_targets(rows, offs, lens, first.astype(jnp.int32)[None], target_ids.reshape(ways, slots))

    own = [compact(rows, way_of, offs, lens, pieces) for pieces in gathered]
    carry = block_product([own], vocab.astype(jnp.int32)[None], proj, tile, None)

    sent = own
    taken = None
    for j in range(1, ring):
        got = [advance(value) for value in sent]
        taken = [swap(value) for value in got]
        sent = [jnp.where(core == 0, t, g) for g, t in zip(got, taken)]
        across = PAIR * ((hop + ring - j + 1) % ring) + (1 - side)
        along = PAIR * ((hop + ring - j) % ring) + side
        blocks = jnp.where(core == 0, jnp.stack([across, along]), jnp.stack([along, across])).astype(jnp.int32)
        carry = block_product([got, taken], blocks, proj, tile, carry)
    sent = [lax.dynamic_slice_in_dim(value, core * half, half, axis=0) for value in taken]
    got = [advance(value) for value in sent]
    taken = [swap(value) for value in got]
    final = PAIR * ((hop + 1) % ring) + (1 - side)
    stats = last_product(got, taken, jnp.stack([final, core]).astype(jnp.int32), proj, tile, carry, targets)

    count = ways * size
    every = lax.all_to_all(jnp.broadcast_to(stats[None], (count,) + stats.shape), AXES, 0, 0)
    top = jnp.max(every[:, 0], axis=0)
    drop = every[:, 0] - top[None]
    scale = jnp.exp(drop)
    total = jnp.sum(scale * every[:, 1], axis=0)
    moment = jnp.sum(scale * (every[:, 2] + every[:, 1] * drop), axis=0)
    picked = jnp.sum(every[:, 3], axis=0)
    log_total = jnp.log(total)
    logprob = picked - top - log_total
    entropy = log_total - moment / total

    row = jnp.arange(rows, dtype=jnp.int32)
    inside = (row[None, :] >= begin[:, None]) & (row[None, :] < (begin + seq_len)[:, None])
    seq_logprob = jnp.sum(jnp.where(inside, logprob[None, :], 0.0), axis=1)
    used = jnp.arange(slots, dtype=jnp.int32) < lens[dp]

    def place(values):
        padded = jnp.concatenate([values, jnp.zeros((slots,), values.dtype)])
        return jnp.where(used, lax.dynamic_slice_in_dim(padded, offs[dp], slots), 0.0)

    return place(logprob), place(entropy), seq_logprob


def solution(mesh):
    placed = (P("dp", "vocab"), P(None, AXES), P(), P(), P())
    return jax.shard_map(
        per_device, mesh=mesh, in_specs=placed, out_specs=(P("dp"), P("dp"), P()), check_vma=False
    )
```

```python
import functools

import jax
import jax.numpy as jnp
from jax import lax
from jax.experimental import pallas as pl
from jax.experimental.pallas import tpu as pltpu
from jax.sharding import PartitionSpec as P


AXES = ("dp", "vocab")
PAIR = 2
LANES = 128
BF16, F32, I32 = jnp.bfloat16, jnp.float32, jnp.int32


def round_up(value, step):
    return -(-value // step) * step


def in_vmem():
    return pl.BlockSpec(memory_space=pltpu.VMEM)


def in_smem():
    return pl.BlockSpec(memory_space=pltpu.SMEM)


def call(kernel, operands, specs, shapes, flops, scratch=(), alias=None, mib=8):
    return pl.pallas_call(
        kernel,
        in_specs=specs,
        out_specs=jax.tree.map(lambda _: in_vmem(), shapes),
        out_shape=shapes,
        scratch_shapes=list(scratch),
        input_output_aliases=alias or {},
        compiler_params=pltpu.CompilerParams(vmem_limit_bytes=mib * 1024 * 1024),
        cost_estimate=pl.CostEstimate(flops=flops, bytes_accessed=1000000, transcendentals=0),
    )(*operands)


def array(shape, dtype):
    return jax.ShapeDtypeStruct(shape, dtype)


def load_kernel(parts, source, out, sems):
    rows = source.shape[0] // parts
    copies = []
    for k in range(parts):
        span = pl.ds(k * rows, rows)
        copy = pltpu.make_async_copy(source.at[span, :], out.at[span, :], sems.at[k])
        copy.start()
        copies.append(copy)
    for copy in copies:
        copy.wait()


def load(proj):
    parts = 16
    specs = [pl.BlockSpec(memory_space=pl.ANY)]
    scratch = [pltpu.SemaphoreType.DMA((parts,))]
    kernel = functools.partial(load_kernel, parts)
    return call(kernel, [proj], specs, array(proj.shape, proj.dtype), 20000000000, scratch)


def place_of(way, seq_len, seq_way):
    start = used = jnp.int32(0)
    for s in range(seq_len.shape[0]):
        start += jnp.where(seq_way[s] < way, seq_len[s], 0)
        used += jnp.where(seq_way[s] == way, seq_len[s], 0)
    return start, used


def hot_rows(rows, slots, start, used):
    row = lax.broadcasted_iota(I32, (rows, slots), 0)
    slot = lax.broadcasted_iota(I32, (rows, slots), 1)
    return (row - slot == start) & (slot < used)


def compact_kernel(seq_len, seq_way, _, *refs):
    pieces, out, mine = refs[:-2], refs[-2], refs[-1]
    rows, slots = out.shape[0], pieces[0].shape[0]
    half = mine.shape[0]
    dp = lax.axis_index("dp")
    spots = lax.axis_size("dp") // PAIR
    spot, core = dp // PAIR, dp % PAIR
    total = None
    for k in range(spots):
        there = lax.rem(spot + spots - k, spots) * PAIR
        for c, piece in zip((core, 1 - core), pieces[PAIR * k : PAIR * k + PAIR]):
            hot = hot_rows(rows, slots, *place_of(there + c, seq_len, seq_way))
            part = jnp.dot(jnp.where(hot, 1.0, 0.0).astype(BF16), piece[...], preferred_element_type=F32)
            total = part if total is None else total + part
    out[...] = total.astype(BF16)
    mine[...] = out[pl.ds(pl.multiple_of(core * half, half), half), :]


def target_kernel(seq_len, seq_way, _, ids, out):
    ways, slots = ids.shape
    rows = out.shape[0]
    total = jnp.zeros((rows, slots), I32)
    for way in range(ways):
        hot = hot_rows(rows, slots, *place_of(way, seq_len, seq_way))
        total += jnp.where(hot, ids[way : way + 1, :], 0)
    out[...] = jnp.broadcast_to(jnp.sum(total, axis=1, keepdims=True), out.shape)


def assemble(left, column, mine, other):
    half, depth = mine.shape
    core = lax.axis_index("dp") % PAIR
    left[pl.ds(pl.multiple_of(core * half, half), half), column : column + depth] = mine[...]
    left[pl.ds(pl.multiple_of((1 - core) * half, half), half), column : column + depth] = other[...]


def weights_of(proj, block, depth, n, wide):
    return proj[pl.ds(pl.multiple_of(block * depth, depth), depth), n : n + wide]


def first_kernel(left, proj, out):
    wide = min(512, out.shape[1])
    for n in range(0, out.shape[1], wide):
        weights = weights_of(proj, lax.axis_index("vocab"), left.shape[1], n, wide)
        out[:, n : n + wide] = jnp.dot(left[...], weights, preferred_element_type=F32)


def ring_block(j):
    vocab, size = lax.axis_index("vocab"), lax.axis_size("vocab")
    return lax.rem(vocab + size - PAIR * j, size)


def across(block):
    return block + 1 - PAIR * lax.rem(block, PAIR)


def block_kernel(j, ring_mine, ring_other, pair_mine, pair_other, proj, carry, out, left):
    depth = ring_mine.shape[1]
    assemble(left, 0, ring_mine, ring_other)
    assemble(left, depth, pair_mine, pair_other)
    wide = min(512, out.shape[1])
    for n in range(0, out.shape[1], wide):
        total = jnp.dot(
            left[:, :depth], weights_of(proj, ring_block(j), depth, n, wide), preferred_element_type=F32
        )
        total += jnp.dot(
            left[:, depth:], weights_of(proj, across(ring_block(j - 1)), depth, n, wide), preferred_element_type=F32
        )
        out[:, n : n + wide] = carry[:, n : n + wide] + total


def last_kernel(j, mine, other, proj, carry, targets, out, left, logits):
    rows, width = carry.shape
    depth = mine.shape[1]
    assemble(left, 0, mine, other)
    wide = min(512, width)
    for n in range(0, width, wide):
        weights = weights_of(proj, across(ring_block(j)), depth, n, wide)
        logits[:, n : n + wide] = carry[:, n : n + wide] + jnp.dot(left[...], weights, preferred_element_type=F32)
    first = (lax.axis_index("dp") * lax.axis_size("vocab") + lax.axis_index("vocab")) * width
    group = 16
    lane = lax.broadcasted_iota(I32, (group, LANES), 1)
    for r in range(0, rows, group):
        band = slice(r, r + group)
        peak = logits[band, :LANES]
        for n in range(LANES, width, LANES):
            peak = jnp.maximum(peak, logits[band, n : n + LANES])
        top = jnp.max(peak, axis=1, keepdims=True)
        wanted = targets[band, :] - first - lane
        total = moment = picked = jnp.zeros((group, LANES), F32)
        for n in range(0, width, LANES):
            value = logits[band, n : n + LANES]
            shifted = value - top
            weight = jnp.exp(shifted)
            total += weight
            moment += weight * shifted
            picked = jnp.where(wanted == n, value, picked)
        packed = jnp.where(lane == 0, top, 0.0)
        packed = jnp.where(lane == 1, jnp.sum(total, axis=1, keepdims=True), packed)
        packed = jnp.where(lane == 2, jnp.sum(moment, axis=1, keepdims=True), packed)
        packed = jnp.where(lane == 3, jnp.sum(picked, axis=1, keepdims=True), packed)
        logits[band, :LANES] = packed
    stats = jnp.transpose(logits[:, :LANES])[: out.shape[1], :]
    out[...] = jnp.broadcast_to(stats[None], out.shape)


def per_device(hidden, proj, target_ids, seq_len, seq_way):
    ways, size = lax.axis_size("dp"), lax.axis_size("vocab")
    slots, depth = hidden.shape
    width = proj.shape[1]
    spots, ring = ways // PAIR, size // PAIR
    kept = slots + (ways - 1) * (5 * slots // 16)
    rows = round_up(kept, 32)
    half = rows // 2

    def permute(value, axis, count, to):
        return lax.ppermute(value, axis, [(i, to(i)) for i in range(count)])

    def swap(value):
        return permute(value, "dp", ways, lambda i: i ^ 1)

    def over_pair(value):
        return permute(value, "vocab", size, lambda i: i ^ 1)

    def over_ring(value):
        return permute(value, "vocab", size, lambda i: (i + PAIR) % size)

    pieces = [hidden, swap(hidden)]
    for k in range(1, spots):
        turned = permute(hidden, "dp", ways, lambda i: (i + k * PAIR) % ways)
        pieces += [turned, swap(turned)]
    ids, proj = lax.optimization_barrier((target_ids.reshape(ways, slots), proj))
    held = load(proj)
    smem = [in_smem(), in_smem()]
    own, mine = call(
        compact_kernel,
        [seq_len, seq_way, held, *pieces],
        smem + [in_vmem()] * (len(pieces) + 1),
        (array((rows, depth), BF16), array((half, depth), BF16)),
        2 * rows * slots * ways * depth,
    )
    targets = call(
        target_kernel, [seq_len, seq_way, held, ids], smem + [in_vmem()] * 2, array((rows, LANES), I32), 1000000
    )
    flops = 2 * rows * depth * width
    carry = call(first_kernel, [own, held], [in_vmem()] * 2, array((rows, width), F32), flops)

    along = mine
    for j in range(1, ring + 1):
        beside = over_pair(along)
        if j == ring:
            break
        along = over_ring(along)
        lefts = [along, swap(along), beside, swap(beside)]
        carry = call(
            functools.partial(block_kernel, j),
            [*lefts, held, carry],
            [in_vmem()] * 6,
            array((rows, width), F32),
            2 * flops,
            [pltpu.VMEM((rows, 2 * depth), BF16)],
            {5: 0},
        )
    count = ways * size
    stats = call(
        functools.partial(last_kernel, ring - 1),
        [beside, swap(beside), held, carry, targets],
        [in_vmem()] * 5,
        array((count, 4, rows), F32),
        flops,
        [pltpu.VMEM((rows, depth), BF16), pltpu.VMEM((rows, width), F32)],
    )

    stats, seq_len, seq_way = lax.optimization_barrier((stats, seq_len, seq_way))
    every = lax.all_to_all(stats, AXES, 0, 0)
    top = jnp.max(every[:, 0], axis=0)
    drop = every[:, 0] - top[None]
    scale = jnp.exp(drop)
    total = jnp.sum(scale * every[:, 1], axis=0)
    moment = jnp.sum(scale * (every[:, 2] + every[:, 1] * drop), axis=0)
    picked = jnp.sum(every[:, 3], axis=0)
    log_total = jnp.log(total)
    logprob = picked - top - log_total
    entropy = log_total - moment / total

    order = jnp.arange(seq_len.shape[0], dtype=I32)
    ahead = (seq_way[None, :] < seq_way[:, None]) | (
        (seq_way[None, :] == seq_way[:, None]) & (order[None, :] < order[:, None])
    )
    begin = jnp.sum(jnp.where(ahead, seq_len[None, :], 0), axis=1)
    dp = lax.axis_index("dp")
    start = jnp.sum(jnp.where(seq_way < dp, seq_len, 0))
    used = jnp.arange(slots, dtype=I32) < jnp.sum(jnp.where(seq_way == dp, seq_len, 0))
    row = jnp.arange(rows, dtype=I32)
    inside = (row[None, :] >= begin[:, None]) & (row[None, :] < (begin + seq_len)[:, None])
    seq_logprob = jnp.sum(jnp.where(inside, logprob[None, :], 0.0), axis=1)

    def place(values):
        padded = jnp.concatenate([values, jnp.zeros((slots,), values.dtype)])
        return jnp.where(used, lax.dynamic_slice_in_dim(padded, start, slots), 0.0)

    return place(logprob), place(entropy), seq_logprob


def solution(mesh):
    placed = (P("dp", "vocab"), P(None, AXES), P(), P(), P())

    return jax.shard_map(per_device, mesh=mesh, in_specs=placed, out_specs=(P("dp"), P("dp"), P()), check_vma=False)
```
